32 devices in a mesh: rows: 4 (over y, x), cols: 8 (over z, core).
Axes of the slice: x: 2, y: 2, z: 4, core: 2. Of those that a mesh axis runs over, the one named last changes fastest.
Arguments:
- factor_u: float32 [4, 2048, 128], P('rows', 'cols'), may hold values from -2 to 2
- factor_v: float32 [8, 512, 128], P('cols', 'rows'), may hold values from -2 to 2
- values: bfloat16 [4, 8, 8, 256, 256], P('rows', 'cols'), may hold values from -6 to 6
- mask_words: int32 [4, 8, 8, 16, 256], P('rows', 'cols'), may hold values from 0 to 65535, as said below
- tile_cols: int32 [4, 8, 8], P('rows', 'cols'), may hold values from 0 to 1
Outputs:
- new_u: float32 [4, 2048, 128], P('rows', 'cols')
- new_v: float32 [8, 512, 128], P('cols', 'rows')
- loss: float32 [], replicated
The draws below stay inside these ranges and needn't reach their ends.
Inputs may be any that keep to these rules, and one draw needn't show every extreme that they name: `mask_words`: bit b of word w of a slot marks the entry in row 16 w + b of the tile.
All inputs are finite; a program needn't handle non-finite values.
Results may differ from the reference program's by a relative error of at most 0.02.
Values may be sent and summed in bfloat16 or wider, within the bound.
A program may use at most 64 MiB of HBM per device.

```python
import jax
import jax.numpy as jnp
from jax import lax

K = 128
TILE = 256
BAND_U = 2048
BAND_V = 512
ROW_TILES = 8
COL_TILES = 2
ENTRIES = 16777216
N_ROWS = 4
N_COLS = 8


def draw_mask_words(key, part):
    level_key = jax.random.fold_in(key, 11)
    ceiling_key = jax.random.fold_in(key, 12)
    bit_key = jax.random.fold_in(key, 13)
    levels = jax.random.randint(level_key, (N_ROWS, N_COLS, ROW_TILES), 0, 9)
    ceiling = jax.random.randint(ceiling_key, (N_ROWS, N_COLS, 1), 3, 10)
    levels = jnp.minimum(levels, ceiling)
    shifts = jnp.arange(16, dtype=jnp.int32)

    def draw_row(row_index):
        samples = jax.random.randint(jax.random.fold_in(bit_key, row_index), (N_COLS, ROW_TILES, TILE // 16, 16, TILE), 0, 8)
        bit_values = (samples < levels[row_index][:, :, None, None, None]).astype(jnp.int32)
        packed = jnp.sum(jnp.left_shift(bit_values, shifts[:, None]), axis=3)
        return packed.astype(jnp.int32)
    return lax.map(draw_row, jnp.arange(N_ROWS, dtype=jnp.int32))


def touch_ends(array, stream_key, least, top_value):
    dims = array.shape
    index_at = [jax.random.randint(jax.random.fold_in(stream_key, axis), (), 0, dims[axis]) for axis in range(len(dims))]
    array = array.at[tuple(index_at)].set(least)
    longest = dims.index(max(dims))
    index_at[longest] = (index_at[longest] + 1) % dims[longest]
    return array.at[tuple(index_at)].set(top_value)


def steps_of(key, shape, split, low, high):
    def one(dim, blocks):
        draws = jax.random.uniform(jax.random.fold_in(jax.random.fold_in(key, 6), dim), (blocks,), jnp.float32, low / len(split), high / len(split))
        return jnp.repeat(jnp.exp(draws), shape[dim] // blocks).reshape((-1,) + (1,) * (len(shape) - dim - 1))

    gain = one(*split[0])
    for cut in split[1:]:
        gain = gain * one(*cut)
    return gain


def gaussian(rng, shape, scale, bound, pieces=(), kind=jnp.bfloat16):
    result = scale * jax.random.normal(rng, shape, jnp.float32)
    if pieces:
        result = result * steps_of(rng, shape, pieces, -0.22, 0.18)
    return jnp.clip(result, -bound, bound).astype(kind)


def setup_inputs(seed: int = 0) -> dict:
    splits = jax.random.split(jax.random.key(seed), 6)
    return {
        "factor_u": gaussian(splits[0], (N_ROWS, BAND_U, K), 0.3, 2.0, ((0, 4), (1, 8)), jnp.float32),
        "factor_v": gaussian(splits[1], (N_COLS, BAND_V, K), 0.3, 2.0, ((0, 8), (1, 4)), jnp.float32),
        "values": gaussian(splits[2], (N_ROWS, N_COLS, ROW_TILES, TILE, TILE), 1.0, 6.0, ((0, 4), (1, 8))),
        "mask_words": draw_mask_words(jax.random.fold_in(splits[5], 71), 0),
        "tile_cols": touch_ends(jax.random.randint(splits[4], (N_ROWS, N_COLS, ROW_TILES), 0, COL_TILES), jax.random.fold_in(splits[4], 1), 0, COL_TILES - 1).astype(jnp.int32),
    }


step_rate = 0.01
ridge_weight = 0.1


def decode(mask_bits):
    shifts = jnp.arange(16, dtype=jnp.int32)
    bit_values = jnp.bitwise_and(jnp.right_shift(mask_bits[..., None, :], shifts[:, None]), 1)
    lead = mask_bits.shape[:-2]
    return bit_values.reshape(lead + (mask_bits.shape[-2] * 16, mask_bits.shape[-1])).astype(jnp.float32)


def rounded(array_in):
    return lax.optimization_barrier(array_in.astype(jnp.bfloat16)).astype(jnp.float32)


def device_terms(left_band, right_band, tile_values, mask_bits, column_ids):
    left_rows = left_band.reshape(-1, TILE, K).astype(jnp.float32)
    right_tiles = right_band.reshape(-1, TILE, K)
    right_rows = jnp.take(right_tiles, column_ids, axis=0).astype(jnp.float32)
    observed = decode(mask_bits)
    predicted = jnp.einsum("sik,sjk->sij", left_rows, right_rows, precision=lax.Precision.HIGHEST)
    residual = observed * (predicted - tile_values.astype(jnp.float32))
    resid_low = rounded(residual)
    grad_rows = jnp.einsum("sij,sjk->sik", resid_low, right_rows, precision=lax.Precision.HIGHEST)
    grad_cols = jnp.einsum("sij,sik->sjk", resid_low, left_rows, precision=lax.Precision.HIGHEST)
    col_sums = jax.ops.segment_sum(grad_cols, column_ids, num_segments=COL_TILES)
    squares = 0.5 * jnp.sum(residual * residual)
    return grad_rows.reshape(-1, K), col_sums.reshape(-1, K), squares


def reference(factor_u, factor_v, values, mask_words, tile_cols):
    u_low = factor_u.astype(jnp.bfloat16)
    v_low = factor_v.astype(jnp.bfloat16)

    def row_group(running, row_index):
        v_total, data_total = running

        def col_group(u_sum, col_index):
            grad_rows, col_sums, squares = device_terms(
                u_low[row_index], v_low[col_index], values[row_index, col_index],
                mask_words[row_index, col_index], tile_cols[row_index, col_index])
            return u_sum + rounded(grad_rows), (rounded(col_sums), squares)

        u_sum, outputs = lax.scan(col_group, jnp.zeros((BAND_U, K), jnp.float32),
                                  jnp.arange(N_COLS, dtype=jnp.int32))
        col_parts, square_parts = outputs
        return (v_total + col_parts, data_total + jnp.sum(square_parts)), u_sum

    initial = (jnp.zeros((N_COLS, BAND_V, K), jnp.float32), jnp.zeros((), jnp.float32))
    finals, grad_u = lax.scan(row_group, initial, jnp.arange(N_ROWS, dtype=jnp.int32))
    grad_v, data_total = finals
    penalty = 0.5 * ridge_weight * (jnp.sum(factor_u * factor_u) + jnp.sum(factor_v * factor_v))
    loss = (data_total + penalty) / ENTRIES
    new_u = factor_u - step_rate * (grad_u + ridge_weight * factor_u)
    new_v = factor_v - step_rate * (grad_v + ridge_weight * factor_v)
    return new_u, new_v, loss
```

```python
import functools

import jax
import jax.numpy as jnp
from jax import lax
from jax.experimental import pallas as pl
from jax.experimental.pallas import tpu as pltpu
from jax.sharding import PartitionSpec as P

step_rate = 0.01
ridge_weight = 0.1
MESH = pl.DeviceIdType.MESH
NT = (((1,), (1,)), ((), ()))
TN = (((0,), (0,)), ((), ()))
WORD = 16


def loop(start, stop, body):
    if stop - start <= 8:
        for i in range(start, stop):
            body(i)
    else:
        lax.fori_loop(start, stop, lambda i, z: (body(i), z)[1], 0)


def fold(x):
    return jnp.sum(x.reshape(x.shape[0] // 8, 8, x.shape[1]), axis=0)


def kernel(
    n_r, n_c, entries,
    u_hbm, v_hbm, val_hbm, mask_hbm, tc_ref,
    nu_ref, nv_ref, loss_ref,
    uf, vf, vals, masks, ub, vb, keep, xsend, pbuf, rsend, rbuf,
    acc, vsend, vrecv, sq, lrow, lcol,
    ld_sem, vg_s, vg_r, ug_s, ug_r, ud_s, ud_r, pd_s, pd_r, pr_s, pr_r,
    vr_s, vr_r, lr_s, lr_r, lc_s, lc_r,
):
    n_q = n_c // 2
    r = lax.axis_index("rows")
    c = lax.axis_index("cols")
    q = c // 2
    a = c % 2
    pc = 2 * q + 1 - a
    tile = vals.shape[1]
    own_v = vf.shape[0]
    per_tile = tile // own_v

    ld_u = pltpu.make_async_copy(u_hbm.at[0], uf, ld_sem.at[0])
    ld_v = pltpu.make_async_copy(v_hbm.at[0], vf, ld_sem.at[1])
    ld_m = pltpu.make_async_copy(mask_hbm.at[0, 0], masks, ld_sem.at[2])
    ld_x = pltpu.make_async_copy(val_hbm.at[0, 0], vals, ld_sem.at[3])
    ld_v.start()
    ld_u.start()
    ld_m.start()
    ld_x.start()

    bar = pltpu.get_barrier_semaphore()

    def greet_row(d):
        pl.semaphore_signal(bar, inc=1, device_id=((r + d) % n_r, c), device_id_type=MESH)

    def greet_col(d):
        pl.semaphore_signal(bar, inc=1, device_id=(r, (c + d) % n_c), device_id_type=MESH)

    loop(1, n_r, greet_row)
    loop(1, n_c, greet_col)

    ld_v.wait()
    vb[r // per_tile, pl.ds(pl.multiple_of((r % per_tile) * own_v, own_v), own_v)] = vf[...].astype(jnp.bfloat16)
    ld_u.wait()
    ub[c] = uf[...].astype(jnp.bfloat16)
    sq[...] = jnp.zeros_like(sq)
    acc[...] = jnp.zeros_like(acc)
    penalty = fold(uf[...] * uf[...]) + fold(vf[...] * vf[...])

    pl.semaphore_wait(bar, n_r + n_c - 2)

    def chunk(i):
        return vb.at[i // per_tile, pl.ds(pl.multiple_of((i % per_tile) * own_v, own_v), own_v)]

    def rdma(src, dst, s, g, dev):
        return pltpu.make_async_remote_copy(
            src_ref=src, dst_ref=dst, send_sem=s, recv_sem=g, device_id=dev, device_id_type=MESH
        )

    def vg(d):
        return rdma(chunk(r), chunk(r), vg_s.at[d], vg_r.at[d], ((r + d) % n_r, c))

    def vg_in(d):
        src = (r + n_r - d) % n_r
        return rdma(chunk(src), chunk(src), vg_s.at[d], vg_r.at[d], ((r + d) % n_r, c))

    def chip(d):
        return (q + n_q - d) % n_q

    def ug(d):
        return rdma(ub.at[c], ub.at[c], ug_s.at[d], ug_r.at[d], (r, 2 * ((q + d) % n_q) + a))

    def ug_in(d):
        s = 2 * chip(d) + a
        return rdma(ub.at[s], ub.at[s], ug_s.at[d], ug_r.at[d], (r, 2 * ((q + d) % n_q) + a))

    def ud(d):
        s = 2 * chip(d) + a
        return rdma(ub.at[s], ub.at[s], ud_s.at[d], ud_r.at[d], (r, pc))

    def ud_in(d):
        s = 2 * chip(d) + 1 - a
        return rdma(ub.at[s], ub.at[s], ud_s.at[d], ud_r.at[d], (r, pc))

    def pd(d):
        return rdma(xsend.at[d], pbuf.at[d], pd_s.at[d], pd_r.at[d], (r, pc))

    def pr(d):
        return rdma(rsend.at[d], rbuf.at[d], pr_s.at[d], pr_r.at[d], (r, 2 * chip(d) + a))

    def vr(d):
        return rdma(vsend.at[(r + d) % n_r], vrecv.at[d], vr_s.at[d], vr_r.at[d], ((r + d) % n_r, c))

    def lr(d):
        return rdma(lrow.at[r], lrow.at[r], lr_s.at[d], lr_r.at[d], ((r + d) % n_r, c))

    def lr_in(d):
        src = (r + n_r - d) % n_r
        return rdma(lrow.at[src], lrow.at[src], lr_s.at[d], lr_r.at[d], ((r + d) % n_r, c))

    def lc(d):
        return rdma(lcol.at[c], lcol.at[c], lc_s.at[d], lc_r.at[d], (r, (c + d) % n_c))

    def lc_in(d):
        src = (c + n_c - d) % n_c
        return rdma(lcol.at[src], lcol.at[src], lc_s.at[d], lc_r.at[d], (r, (c + d) % n_c))

    loop(1, n_r, lambda d: vg(d).start())
    ud(0).start()
    loop(1, n_q, lambda d: ug(d).start())

    ld_m.wait()
    ld_x.wait()
    loop(1, n_r, lambda d: vg_in(d).wait_recv())

    bits = lax.shift_left(jnp.int32(1), lax.broadcasted_iota(jnp.int32, (1, WORD, tile), 1))

    def slot(s, put):
        left = ub[s]
        which = tc_ref[0, 0, s]
        right = vb[which]
        predicted = lax.dot_general(left, right, NT, preferred_element_type=jnp.float32)
        words = masks[s]
        seen = (jnp.broadcast_to(words[:, None, :], (tile // WORD, WORD, tile)) & bits).reshape(tile, tile) != 0
        residual = jnp.where(seen, predicted - vals[s].astype(jnp.float32), 0.0)
        low = residual.astype(jnp.bfloat16)
        put(jnp.dot(low, right, preferred_element_type=jnp.float32))
        sq[...] += fold(residual * residual)
        cols_t = lax.dot_general(left, low, TN, preferred_element_type=jnp.float32)
        for t in range(acc.shape[0]):
            acc[t] += cols_t * (which == t).astype(jnp.float32)

    def put_keep(d):
        def put(x):
            keep[d] = x
        return put

    def put_send(d):
        def put(x):
            xsend[d] = x.astype(jnp.bfloat16)
        return put

    def stage_c(d):
        pd(d).wait_recv()
        rsend[d] = (keep[d] + pbuf[d].astype(jnp.float32)).astype(jnp.bfloat16)
        pr(d).start()

    def stage_a(d):
        ug_in(d).wait_recv()
        ud(d).start()
        slot(2 * chip(d) + a, put_keep(d))

    def stage_b(d):
        ud_in(d).wait_recv()
        slot(2 * chip(d) + 1 - a, put_send(d))
        pd(d).start()

    slot(c, put_keep(0))
    stage_b(0)
    stage_a(1)
    stage_b(1)

    def step(d):
        stage_a(d)
        stage_c(d - 1)
        stage_b(d)

    loop(2, n_q, step)

    half = sq.shape[1] // 2
    lrow[r] = 0.5 * (sq[:, :half] + sq[:, half:]) + 0.5 * ridge_weight * penalty

    for t in range(acc.shape[0]):
        whole = acc[t].T.astype(jnp.bfloat16)
        for h in range(per_tile):
            vsend[t * per_tile + h] = whole[h * own_v:(h + 1) * own_v]
    loop(1, n_r, lambda d: lr(d).start())
    loop(1, n_r, lambda d: vr(d).start())
    stage_c(n_q - 1)

    loop(1, n_r, lambda d: lr_in(d).wait_recv())
    total = lrow[0]
    for i in range(1, n_r):
        total = total + lrow[i]
    lcol[c] = total
    pd(0).wait_recv()
    keep[0] = keep[0] + pbuf[0].astype(jnp.float32)
    loop(1, n_c, lambda d: lc(d).start())

    def add_v(d):
        vr(d).wait_recv()
        vf_sum[...] += vrecv[d].astype(jnp.float32)

    vf_sum = nv_ref.at[0]
    vf_sum[...] = vsend[r].astype(jnp.float32)
    loop(1, n_r, add_v)
    vf_sum[...] = vf[...] - step_rate * (vf_sum[...] + ridge_weight * vf[...])

    def add_u(d):
        pr(d).wait_recv()
        keep[0] += rbuf[d].astype(jnp.float32)

    loop(1, n_q, add_u)
    nu_ref[0] = uf[...] - step_rate * (keep[0] + ridge_weight * uf[...])

    loop(1, n_c, lambda d: lc_in(d).wait_recv())
    total = lcol[0]
    for i in range(1, n_c):
        total = total + lcol[i]
    loss_ref[...] = jnp.sum(jnp.sum(total, axis=1, keepdims=True), axis=0, keepdims=True) / entries

    def drain_q(d):
        ud(d).wait_send()
        pd(d).wait_send()

    def drain_q1(d):
        ug(d).wait_send()
        pr(d).wait_send()

    def drain_r(d):
        vg(d).wait_send()
        vr(d).wait_send()
        lr(d).wait_send()

    loop(0, n_q, drain_q)
    loop(1, n_q, drain_q1)
    loop(1, n_r, drain_r)
    loop(1, n_c, lambda d: lc(d).wait_send())


def per_device(n_r, n_c, factor_u, factor_v, values, mask_words, tile_cols):
    _, own_u, rank = factor_u.shape
    own_v = factor_v.shape[1]
    slots, tile = values.shape[2], values.shape[3]
    n_q = n_c // 2
    entries = n_r * n_c * slots * tile * tile
    col_tiles = n_r * own_v // tile
    dma = pltpu.SemaphoreType.DMA
    bf, f32 = jnp.bfloat16, jnp.float32
    anym = pl.BlockSpec(memory_space=pl.ANY)
    vm = pl.BlockSpec(memory_space=pltpu.VMEM)
    new_u, new_v, loss = pl.pallas_call(
        functools.partial(kernel, n_r, n_c, float(entries)),
        out_shape=(
            jax.ShapeDtypeStruct(factor_u.shape, f32),
            jax.ShapeDtypeStruct(factor_v.shape, f32),
            jax.ShapeDtypeStruct((1, 1), f32),
        ),
        in_specs=[anym, anym, anym, anym, pl.BlockSpec(memory_space=pltpu.SMEM)],
        out_specs=(vm, vm, vm),
        scratch_shapes=[
            pltpu.VMEM((own_u, rank), f32),
            pltpu.VMEM((own_v, rank), f32),
            pltpu.VMEM(values.shape[2:], bf),
            pltpu.VMEM(mask_words.shape[2:], jnp.int32),
            pltpu.VMEM((n_c, own_u, rank), bf),
            pltpu.VMEM((col_tiles, tile, rank), bf),
            pltpu.VMEM((n_q, own_u, rank), f32),
            pltpu.VMEM((n_q, own_u, rank), bf),
            pltpu.VMEM((n_q, own_u, rank), bf),
            pltpu.VMEM((n_q, own_u, rank), bf),
            pltpu.VMEM((n_q, own_u, rank), bf),
            pltpu.VMEM((col_tiles, rank, tile), f32),
            pltpu.VMEM((n_r, own_v, rank), bf),
            pltpu.VMEM((n_r, own_v, rank), bf),
            pltpu.VMEM((8, tile), f32),
            pltpu.VMEM((n_r, 8, tile // 2), f32),
            pltpu.VMEM((n_c, 8, tile // 2), f32),
            dma((4,)),
            dma((n_r,)), dma((n_r,)),
            dma((n_q,)), dma((n_q,)),
            dma((n_q,)), dma((n_q,)),
            dma((n_q,)), dma((n_q,)),
            dma((n_q,)), dma((n_q,)),
            dma((n_r,)), dma((n_r,)),
            dma((n_r,)), dma((n_r,)),
            dma((n_c,)), dma((n_c,)),
        ],
        compiler_params=pltpu.CompilerParams(collective_id=0, has_side_effects=True),
    )(factor_u, factor_v, values, mask_words, tile_cols)
    return new_u, new_v, loss[0, 0]


def solution(mesh):
    n_r, n_c = mesh.shape["rows"], mesh.shape["cols"]
    in_specs = (
        P("rows", "cols", None),
        P("cols", "rows", None),
        P("rows", "cols", None, None, None),
        P("rows", "cols", None, None, None),
        P("rows", "cols", None),
    )
    out_specs = (P("rows", "cols", None), P("cols", "rows", None), P())
    return jax.shard_map(
        functools.partial(per_device, n_r, n_c),
        mesh=mesh, in_specs=in_specs, out_specs=out_specs, check_vma=False,
    )
```

```python
import functools

import jax
import jax.numpy as jnp
from jax import lax
from jax.experimental import pallas as pl
from jax.experimental.pallas import tpu as pltpu
from jax.sharding import PartitionSpec as P

step_rate = 0.01
ridge_weight = 0.1
MESH = pl.DeviceIdType.MESH
NT = (((1,), (1,)), ((), ()))
TN = (((0,), (0,)), ((), ()))
WORD = 16
CUTS = 2


def loop(start, stop, body):
    if stop - start <= 8:
        for i in range(start, stop):
            body(i)
    else:
        lax.fori_loop(start, stop, lambda i, z: (body(i), z)[1], 0)


def fold(x):
    return jnp.sum(x.reshape(x.shape[0] // 8, 8, x.shape[1]), axis=0)


def kernel(
    n_r, n_c, entries,
    u_hbm, v_hbm, val_hbm, mask_hbm, tc_ref,
    nu_ref, nv_ref, loss_ref,
    uf, vf, vals, masks, ub, vb, keep, xsend, pbuf, rsend, rbuf,
    acc, vsend, vrecv, sq, lrow, lcol,
    ld_sem, vg_s, vg_r, up_s, dn_s, ug_r, ud_s, ud_r, pd_s, pd_r, pr_s, pr_r,
    vr_s, vr_r, lr_s, lr_r, lc_s, lc_r,
):
    n_q = n_c // 2
    r = lax.axis_index("rows")
    c = lax.axis_index("cols")
    q = c // 2
    a = c % 2
    pc = 2 * q + 1 - a
    tile = vals.shape[1]
    own_v = vf.shape[0]
    part = tile // CUTS
    per_tile = tile // own_v

    ld_u = pltpu.make_async_copy(u_hbm.at[0], uf, ld_sem.at[0])
    ld_v = pltpu.make_async_copy(v_hbm.at[0], vf, ld_sem.at[1])
    ld_m = pltpu.make_async_copy(mask_hbm.at[0, 0], masks, ld_sem.at[2])
    ld_x = pltpu.make_async_copy(val_hbm.at[0, 0], vals, ld_sem.at[3])
    ld_v.start()
    ld_u.start()
    ld_m.start()
    ld_x.start()

    bar = pltpu.get_barrier_semaphore()

    def greet(dev):
        pl.semaphore_signal(bar, inc=1, device_id=dev, device_id_type=MESH)

    def chain_greet():
        greet((r, pc))
        pl.when(q > 0)(lambda: greet((r, c - 2)))
        pl.when(q < n_q - 1)(lambda: greet((r, c + 2)))

    chain_greet()
    loop(1, n_r, lambda d: greet(((r + d) % n_r, c)))

    ld_v.wait()
    vb[r // per_tile, pl.ds(pl.multiple_of((r % per_tile) * own_v, own_v), own_v)] = vf[...].astype(jnp.bfloat16)
    ld_u.wait()
    ub[c] = uf[...].astype(jnp.bfloat16)
    sq[...] = jnp.zeros_like(sq)
    acc[...] = jnp.zeros_like(acc)
    penalty = fold(uf[...] * uf[...]) + fold(vf[...] * vf[...])

    beside = (q + n_q - 1) // n_q + (2 * n_q - 2 - q) // n_q
    pl.semaphore_wait(bar, n_r + beside)

    def chunk(i):
        return vb.at[i // per_tile, pl.ds(pl.multiple_of((i % per_tile) * own_v, own_v), own_v)]

    def rdma(src, dst, s, g, dev):
        return pltpu.make_async_remote_copy(
            src_ref=src, dst_ref=dst, send_sem=s, recv_sem=g, device_id=dev, device_id_type=MESH
        )

    def vg(d):
        return rdma(chunk(r), chunk(r), vg_s.at[d], vg_r.at[d], ((r + d) % n_r, c))

    def vg_in(d):
        src = (r + n_r - d) % n_r
        return rdma(chunk(src), chunk(src), vg_s.at[d], vg_r.at[d], ((r + d) % n_r, c))

    def piece(s, k):
        return ub.at[s, pl.ds(k * part, part)]

    def up(t, k):
        s = 2 * t + a
        return rdma(piece(s, k), piece(s, k), up_s.at[t, k], ug_r.at[t, k], (r, c + 2))

    def down(t, k):
        s = 2 * t + a
        return rdma(piece(s, k), piece(s, k), dn_s.at[t, k], ug_r.at[t, k], (r, c - 2))

    def ud(t, k):
        s = 2 * t + a
        return rdma(piece(s, k), piece(s, k), ud_s.at[t, k], ud_r.at[t, k], (r, pc))

    def ud_in(t, k):
        s = 2 * t + 1 - a
        return rdma(piece(s, k), piece(s, k), ud_s.at[t, k], ud_r.at[t, k], (r, pc))

    def pd(t):
        return rdma(xsend.at[t], pbuf.at[t], pd_s.at[t], pd_r.at[t], (r, pc))

    def pr(t):
        return rdma(rsend.at[t], rbuf.at[q], pr_s.at[t], pr_r.at[q], (r, 2 * t + a))

    def pr_in(t):
        return rdma(rsend.at[t], rbuf.at[t], pr_s.at[t], pr_r.at[t], (r, 2 * t + a))

    def vr(d):
        return rdma(vsend.at[(r + d) % n_r], vrecv.at[d], vr_s.at[d], vr_r.at[d], ((r + d) % n_r, c))

    def lr(d):
        return rdma(lrow.at[r], lrow.at[r], lr_s.at[d], lr_r.at[d], ((r + d) % n_r, c))

    def lr_in(d):
        src = (r + n_r - d) % n_r
        return rdma(lrow.at[src], lrow.at[src], lr_s.at[d], lr_r.at[d], ((r + d) % n_r, c))

    def lc(d):
        return rdma(lcol.at[c], lcol.at[c], lc_s.at[d], lc_r.at[d], (r, (c + d) % n_c))

    def lc_in(d):
        src = (c + n_c - d) % n_c
        return rdma(lcol.at[src], lcol.at[src], lc_s.at[d], lc_r.at[d], (r, (c + d) % n_c))

    def open_chain(k):
        pl.when(q > 0)(lambda: down(q, k).start())
        pl.when(q < n_q - 1)(lambda: up(q, k).start())
        ud(q, k).start()

    loop(0, CUTS, open_chain)
    loop(1, n_r, lambda d: vg(d).start())

    def forward(h):
        def below(k):
            up(q - h, k).wait_recv()
            pl.when(q < n_q - 1)(lambda: up(q - h, k).start())
            ud(q - h, k).start()

        def above(k):
            down(q + h, k).wait_recv()
            pl.when(q > 0)(lambda: down(q + h, k).start())
            ud(q + h, k).start()

        for k in range(CUTS):
            pl.when(q >= h)(functools.partial(below, k))
            pl.when(q + h < n_q)(functools.partial(above, k))

    forward(1)
    ld_m.wait()
    ld_x.wait()
    loop(1, n_r, lambda d: vg_in(d).wait_recv())

    bits = lax.shift_left(jnp.int32(1), lax.broadcasted_iota(jnp.int32, (1, WORD, tile), 1))

    def slot(s, put):
        left = ub[s]
        which = tc_ref[0, 0, s]
        right = vb[which]
        predicted = lax.dot_general(left, right, NT, preferred_element_type=jnp.float32)
        words = masks[s]
        seen = (jnp.broadcast_to(words[:, None, :], (tile // WORD, WORD, tile)) & bits).reshape(tile, tile) != 0
        residual = jnp.where(seen, predicted - vals[s].astype(jnp.float32), 0.0)
        low = residual.astype(jnp.bfloat16)
        put(jnp.dot(low, right, preferred_element_type=jnp.float32))
        sq[...] += fold(residual * residual)
        cols_t = lax.dot_general(left, low, TN, preferred_element_type=jnp.float32)
        for t in range(acc.shape[0]):
            acc[t] += cols_t * (which == t).astype(jnp.float32)

    def put_keep(t):
        def put(x):
            keep[t] = x
        return put

    def put_send(t):
        def put(x):
            xsend[t] = x.astype(jnp.bfloat16)
        return put

    def both(t):
        slot(2 * t + a, put_keep(t))
        for k in range(CUTS):
            ud_in(t, k).wait_recv()
        slot(2 * t + 1 - a, put_send(t))
        pd(t).start()

    def pass_on(t):
        pd(t).wait_recv()
        rsend[t] = (keep[t] + pbuf[t].astype(jnp.float32)).astype(jnp.bfloat16)
        pr(t).start()

    def sides(h, what):
        pl.when(q >= h)(lambda: what(q - h))
        pl.when(q + h < n_q)(lambda: what(q + h))

    both(q)
    sides(1, both)

    def step(h):
        forward(h)
        sides(h - 1, pass_on)
        sides(h, both)

    loop(2, n_q, step)

    half = sq.shape[1] // 2
    lrow[r] = 0.5 * (sq[:, :half] + sq[:, half:]) + 0.5 * ridge_weight * penalty

    for t in range(acc.shape[0]):
        whole = acc[t].T.astype(jnp.bfloat16)
        for h in range(per_tile):
            vsend[t * per_tile + h] = whole[h * own_v:(h + 1) * own_v]
    loop(1, n_r, lambda d: lr(d).start())
    loop(1, n_r, lambda d: vr(d).start())
    sides(n_q - 1, pass_on)

    loop(1, n_r, lambda d: lr_in(d).wait_recv())
    total = lrow[0]
    for i in range(1, n_r):
        total = total + lrow[i]
    lcol[c] = total
    pd(q).wait_recv()
    keep[q] = keep[q] + pbuf[q].astype(jnp.float32)
    loop(1, n_c, lambda d: lc(d).start())

    def add_v(d):
        vr(d).wait_recv()
        vf_sum[...] += vrecv[d].astype(jnp.float32)

    vf_sum = nv_ref.at[0]
    vf_sum[...] = vsend[r].astype(jnp.float32)
    loop(1, n_r, add_v)
    vf_sum[...] = vf[...] - step_rate * (vf_sum[...] + ridge_weight * vf[...])

    def add_u(d):
        t = (q + d) % n_q
        pr_in(t).wait_recv()
        keep[q] += rbuf[t].astype(jnp.float32)

    loop(1, n_q, add_u)
    nu_ref[0] = uf[...] - step_rate * (keep[q] + ridge_weight * uf[...])

    loop(1, n_c, lambda d: lc_in(d).wait_recv())
    total = lcol[0]
    for i in range(1, n_c):
        total = total + lcol[i]
    loss_ref[...] = jnp.sum(jnp.sum(total, axis=1, keepdims=True), axis=0, keepdims=True) / entries

    def drain_q(t):
        pd(t).wait_send()
        for k in range(CUTS):
            ud(t, k).wait_send()
            pl.when(jnp.logical_and(t <= q, q < n_q - 1))(lambda: up(t, k).wait_send())
            pl.when(jnp.logical_and(t >= q, q > 0))(lambda: down(t, k).wait_send())

    def drain_q1(d):
        pr((q + d) % n_q).wait_send()

    def drain_r(d):
        vg(d).wait_send()
        vr(d).wait_send()
        lr(d).wait_send()

    loop(0, n_q, drain_q)
    loop(1, n_q, drain_q1)
    loop(1, n_r, drain_r)
    loop(1, n_c, lambda d: lc(d).wait_send())


def per_device(n_r, n_c, factor_u, factor_v, values, mask_words, tile_cols):
    _, own_u, rank = factor_u.shape
    own_v = factor_v.shape[1]
    slots, tile = values.shape[2], values.shape[3]
    n_q = n_c // 2
    entries = n_r * n_c * slots * tile * tile
    col_tiles = n_r * own_v // tile
    dma = pltpu.SemaphoreType.DMA
    bf, f32 = jnp.bfloat16, jnp.float32
    anym = pl.BlockSpec(memory_space=pl.ANY)
    vm = pl.BlockSpec(memory_space=pltpu.VMEM)
    new_u, new_v, loss = pl.pallas_call(
        functools.partial(kernel, n_r, n_c, float(entries)),
        out_shape=(
            pltpu.VMEM(factor_u.shape, f32),
            pltpu.VMEM(factor_v.shape, f32),
            jax.ShapeDtypeStruct((1, 1), f32),
        ),
        in_specs=[anym, anym, anym, anym, pl.BlockSpec(memory_space=pltpu.SMEM)],
        out_specs=(vm, vm, vm),
        scratch_shapes=[
            pltpu.VMEM((own_u, rank), f32),
            pltpu.VMEM((own_v, rank), f32),
            pltpu.VMEM(values.shape[2:], bf),
            pltpu.VMEM(mask_words.shape[2:], jnp.int32),
            pltpu.VMEM((n_c, own_u, rank), bf),
            pltpu.VMEM((col_tiles, tile, rank), bf),
            pltpu.VMEM((n_q, own_u, rank), f32),
            pltpu.VMEM((n_q, own_u, rank), bf),
            pltpu.VMEM((n_q, own_u, rank), bf),
            pltpu.VMEM((n_q, own_u, rank), bf),
            pltpu.VMEM((n_q, own_u, rank), bf),
            pltpu.VMEM((col_tiles, rank, tile), f32),
            pltpu.VMEM((n_r, own_v, rank), bf),
            pltpu.VMEM((n_r, own_v, rank), bf),
            pltpu.VMEM((8, tile), f32),
            pltpu.VMEM((n_r, 8, tile // 2), f32),
            pltpu.VMEM((n_c, 8, tile // 2), f32),
            dma((4,)),
            dma((n_r,)), dma((n_r,)),
            dma((n_q, CUTS)), dma((n_q, CUTS)), dma((n_q, CUTS)),
            dma((n_q, CUTS)), dma((n_q, CUTS)),
            dma((n_q,)), dma((n_q,)),
            dma((n_q,)), dma((n_q,)),
            dma((n_r,)), dma((n_r,)),
            dma((n_r,)), dma((n_r,)),
            dma((n_c,)), dma((n_c,)),
        ],
        compiler_params=pltpu.CompilerParams(collective_id=0, has_side_effects=True),
    )(factor_u, factor_v, values, mask_words, tile_cols)
    return new_u, new_v, loss[0, 0]


def solution(mesh):
    n_r, n_c = mesh.shape["rows"], mesh.shape["cols"]
    in_specs = (
        P("rows", "cols", None),
        P("cols", "rows", None),
        P("rows", "cols", None, None, None),
        P("rows", "cols", None, None, None),
        P("rows", "cols", None),
    )
    out_specs = (P("rows", "cols", None), P("cols", "rows", None), P())
    return jax.shard_map(
        functools.partial(per_device, n_r, n_c),
        mesh=mesh, in_specs=in_specs, out_specs=out_specs, check_vma=False,
    )
```

```python
import functools

import jax
import jax.numpy as jnp
from jax import lax
from jax.experimental import pallas as pl
from jax.experimental.pallas import tpu as pltpu
from jax.sharding import PartitionSpec as P

step_rate = 0.01
ridge_weight = 0.1
MESH = pl.DeviceIdType.MESH
NT = (((1,), (1,)), ((), ()))
TN = (((0,), (0,)), ((), ()))
WORD = 16
CUTS = 2


def loop(start, stop, body):
    if stop - start <= 8:
        for i in range(start, stop):
            body(i)
    else:
        lax.fori_loop(start, stop, lambda i, z: (body(i), z)[1], 0)


def fold(x):
    return jnp.sum(x.reshape(x.shape[0] // 8, 8, x.shape[1]), axis=0)


def kernel(
    n_r, n_c, entries,
    u_hbm, v_hbm, val_hbm, mask_hbm, tc_ref,
    nu_ref, nv_ref, loss_ref,
    uf, vf, vals, masks, ub, vb, keep, xsend, pbuf, rsend, rbuf,
    acc, vsend, vrecv, sq, lrow, lcol,
    ld_sem, vg_s, vg_r, up_s, dn_s, ug_r, ud_s, ud_r, pd_s, pd_r, pr_s, pr_r,
    vr_s, vr_r, lr_s, lr_r, lc_s, lc_r,
):
    n_q = n_c // 2
    r = lax.axis_index("rows")
    c = lax.axis_index("cols")
    q = c // 2
    a = c % 2
    pc = 2 * q + 1 - a
    tile = vals.shape[1]
    own_v = vf.shape[0]
    part = tile // CUTS
    per_tile = tile // own_v

    ld_u = pltpu.make_async_copy(u_hbm.at[0], uf, ld_sem.at[0])
    ld_v = pltpu.make_async_copy(v_hbm.at[0], vf, ld_sem.at[1])
    ld_m = pltpu.make_async_copy(mask_hbm.at[0, 0], masks, ld_sem.at[2])
    ld_x = pltpu.make_async_copy(val_hbm.at[0, 0], vals, ld_sem.at[3])
    ld_v.start()
    ld_u.start()
    ld_m.start()
    ld_x.start()

    bar = pltpu.get_barrier_semaphore()

    def greet(dev):
        pl.semaphore_signal(bar, inc=1, device_id=dev, device_id_type=MESH)

    def chain_greet():
        greet((r, pc))
        pl.when(q > 0)(lambda: greet((r, c - 2)))
        pl.when(q < n_q - 1)(lambda: greet((r, c + 2)))

    chain_greet()
    loop(1, n_r, lambda d: greet(((r + d) % n_r, c)))

    ld_v.wait()
    vb[r // per_tile, pl.ds(pl.multiple_of((r % per_tile) * own_v, own_v), own_v)] = vf[...].astype(jnp.bfloat16)
    ld_u.wait()
    ub[c] = uf[...].astype(jnp.bfloat16)
    sq[...] = jnp.zeros_like(sq)
    acc[...] = jnp.zeros_like(acc)
    penalty = fold(uf[...] * uf[...]) + fold(vf[...] * vf[...])

    beside = (q + n_q - 1) // n_q + (2 * n_q - 2 - q) // n_q
    pl.semaphore_wait(bar, n_r + beside)

    def chunk(i):
        return vb.at[i // per_tile, pl.ds(pl.multiple_of((i % per_tile) * own_v, own_v), own_v)]

    def rdma(src, dst, s, g, dev):
        return pltpu.make_async_remote_copy(
            src_ref=src, dst_ref=dst, send_sem=s, recv_sem=g, device_id=dev, device_id_type=MESH
        )

    def vg(d):
        return rdma(chunk(r), chunk(r), vg_s.at[d], vg_r.at[d], ((r + d) % n_r, c))

    def vg_in(d):
        src = (r + n_r - d) % n_r
        return rdma(chunk(src), chunk(src), vg_s.at[d], vg_r.at[d], ((r + d) % n_r, c))

    def piece(s, k):
        return ub.at[s, pl.ds(k * part, part)]

    def up(t, k):
        s = 2 * t + a
        return rdma(piece(s, k), piece(s, k), up_s.at[t, k], ug_r.at[t, k], (r, c + 2))

    def down(t, k):
        s = 2 * t + a
        return rdma(piece(s, k), piece(s, k), dn_s.at[t, k], ug_r.at[t, k], (r, c - 2))

    def ud(t, k):
        s = 2 * t + a
        return rdma(piece(s, k), piece(s, k), ud_s.at[t, k], ud_r.at[t, k], (r, pc))

    def ud_in(t, k):
        s = 2 * t + 1 - a
        return rdma(piece(s, k), piece(s, k), ud_s.at[t, k], ud_r.at[t, k], (r, pc))

    def pd(t):
        return rdma(xsend.at[t], pbuf.at[t], pd_s.at[t], pd_r.at[t], (r, pc))

    def pr(t):
        return rdma(rsend.at[t], rbuf.at[q], pr_s.at[t], pr_r.at[q], (r, 2 * t + a))

    def pr_in(t):
        return rdma(rsend.at[t], rbuf.at[t], pr_s.at[t], pr_r.at[t], (r, 2 * t + a))

    def vr(d):
        return rdma(vsend.at[(r + d) % n_r], vrecv.at[d], vr_s.at[d], vr_r.at[d], ((r + d) % n_r, c))

    def lr(d):
        return rdma(lrow.at[r], lrow.at[r], lr_s.at[d], lr_r.at[d], ((r + d) % n_r, c))

    def lr_in(d):
        src = (r + n_r - d) % n_r
        return rdma(lrow.at[src], lrow.at[src], lr_s.at[d], lr_r.at[d], ((r + d) % n_r, c))

    def lc(d):
        return rdma(lcol.at[c], lcol.at[c], lc_s.at[d], lc_r.at[d], (r, (c + d) % n_c))

    def lc_in(d):
        src = (c + n_c - d) % n_c
        return rdma(lcol.at[src], lcol.at[src], lc_s.at[d], lc_r.at[d], (r, (c + d) % n_c))

    def open_chain(k):
        pl.when(q > 0)(lambda: down(q, k).start())
        pl.when(q < n_q - 1)(lambda: up(q, k).start())
        ud(q, k).start()

    loop(0, CUTS, open_chain)
    loop(1, n_r, lambda d: vg(d).start())

    def forward(h):
        def below(k):
            up(q - h, k).wait_recv()
            pl.when(q < n_q - 1)(lambda: up(q - h, k).start())
            ud(q - h, k).start()

        def above(k):
            down(q + h, k).wait_recv()
            pl.when(q > 0)(lambda: down(q + h, k).start())
            ud(q + h, k).start()

        for k in range(CUTS):
            pl.when(q >= h)(functools.partial(below, k))
            pl.when(q + h < n_q)(functools.partial(above, k))

    forward(1)
    ld_m.wait()
    ld_x.wait()
    loop(1, n_r, lambda d: vg_in(d).wait_recv())

    bits = lax.shift_left(jnp.int32(1), lax.broadcasted_iota(jnp.int32, (1, WORD, tile), 1))

    def slot(s, put):
        left = ub[s]
        which = tc_ref[0, 0, s]
        right = vb[which]
        predicted = lax.dot_general(left, right, NT, preferred_element_type=jnp.float32)
        words = masks[s]
        seen = (jnp.broadcast_to(words[:, None, :], (tile // WORD, WORD, tile)) & bits).reshape(tile, tile) != 0
        residual = jnp.where(seen, predicted - vals[s].astype(jnp.float32), 0.0)
        low = residual.astype(jnp.bfloat16)
        put(jnp.dot(low, right, preferred_element_type=jnp.float32))
        sq[...] += fold(residual * residual)
        cols_t = lax.dot_general(left, low, TN, preferred_element_type=jnp.float32)
        for t in range(acc.shape[0]):
            acc[t] += cols_t * (which == t).astype(jnp.float32)

    def put_keep(t):
        def put(x):
            keep[t] = x
        return put

    def put_send(t):
        def put(x):
            xsend[t] = x.astype(jnp.bfloat16)
        return put

    def both(t):
        slot(2 * t + a, put_keep(t))
        for k in range(CUTS):
            ud_in(t, k).wait_recv()
        slot(2 * t + 1 - a, put_send(t))
        pd(t).start()

    def pass_on(t):
        pd(t).wait_recv()
        rsend[t] = (keep[t] + pbuf[t].astype(jnp.float32)).astype(jnp.bfloat16)
        pr(t).start()

    def sides(h, what):
        pl.when(q >= h)(lambda: what(q - h))
        pl.when(q + h < n_q)(lambda: what(q + h))

    both(q)
    sides(1, both)

    def step(h):
        forward(h)
        sides(h - 1, pass_on)
        sides(h, both)

    loop(2, n_q, step)

    half = sq.shape[1] // 2
    lrow[r] = 0.5 * (sq[:, :half] + sq[:, half:]) + 0.5 * ridge_weight * penalty

    def finish_tile(t):
        whole = acc[t].T.astype(jnp.bfloat16)
        for h in range(per_tile):
            vsend[t * per_tile + h] = whole[h * own_v:(h + 1) * own_v]

    finish_tile(0)
    loop(1, n_r, lambda d: lr(d).start())
    loop(1, acc.shape[0], finish_tile)
    loop(1, n_r, lambda d: vr(d).start())
    sides(n_q - 1, pass_on)

    loop(1, n_r, lambda d: lr_in(d).wait_recv())
    total = lrow[0]
    for i in range(1, n_r):
        total = total + lrow[i]
    lcol[c] = total
    pd(q).wait_recv()
    keep[q] = keep[q] + pbuf[q].astype(jnp.float32)
    loop(1, n_c, lambda d: lc(d).start())

    def add_v(d):
        vr(d).wait_recv()
        vf_sum[...] += vrecv[d].astype(jnp.float32)

    vf_sum = nv_ref.at[0]
    vf_sum[...] = vsend[r].astype(jnp.float32)
    loop(1, n_r, add_v)
    vf_sum[...] = vf[...] - step_rate * (vf_sum[...] + ridge_weight * vf[...])

    def add_u(d):
        t = (q + d) % n_q
        pr_in(t).wait_recv()
        keep[q] += rbuf[t].astype(jnp.float32)

    loop(1, n_q, add_u)
    nu_ref[0] = uf[...] - step_rate * (keep[q] + ridge_weight * uf[...])

    loop(1, n_c, lambda d: lc_in(d).wait_recv())
    total = lcol[0]
    for i in range(1, n_c):
        total = total + lcol[i]
    loss_ref[...] = jnp.sum(jnp.sum(total, axis=1, keepdims=True), axis=0, keepdims=True) / entries

    def drain_q(t):
        pd(t).wait_send()
        for k in range(CUTS):
            ud(t, k).wait_send()
            pl.when(jnp.logical_and(t <= q, q < n_q - 1))(lambda: up(t, k).wait_send())
            pl.when(jnp.logical_and(t >= q, q > 0))(lambda: down(t, k).wait_send())

    def drain_q1(d):
        pr((q + d) % n_q).wait_send()

    def drain_r(d):
        vg(d).wait_send()
        vr(d).wait_send()
        lr(d).wait_send()

    loop(0, n_q, drain_q)
    loop(1, n_q, drain_q1)
    loop(1, n_r, drain_r)
    loop(1, n_c, lambda d: lc(d).wait_send())


def per_device(n_r, n_c, factor_u, factor_v, values, mask_words, tile_cols):
    _, own_u, rank = factor_u.shape
    own_v = factor_v.shape[1]
    slots, tile = values.shape[2], values.shape[3]
    n_q = n_c // 2
    entries = n_r * n_c * slots * tile * tile
    col_tiles = n_r * own_v // tile
    dma = pltpu.SemaphoreType.DMA
    bf, f32 = jnp.bfloat16, jnp.float32
    anym = pl.BlockSpec(memory_space=pl.ANY)
    vm = pl.BlockSpec(memory_space=pltpu.VMEM)
    new_u, new_v, loss = pl.pallas_call(
        functools.partial(kernel, n_r, n_c, float(entries)),
        out_shape=(
            pltpu.VMEM(factor_u.shape, f32),
            pltpu.VMEM(factor_v.shape, f32),
            pltpu.VMEM((1, 1), f32),
        ),
        in_specs=[anym, anym, anym, anym, pl.BlockSpec(memory_space=pltpu.SMEM)],
        out_specs=(vm, vm, vm),
        scratch_shapes=[
            pltpu.VMEM((own_u, rank), f32),
            pltpu.VMEM((own_v, rank), f32),
            pltpu.VMEM(values.shape[2:], bf),
            pltpu.VMEM(mask_words.shape[2:], jnp.int32),
            pltpu.VMEM((n_c, own_u, rank), bf),
            pltpu.VMEM((col_tiles, tile, rank), bf),
            pltpu.VMEM((n_q, own_u, rank), f32),
            pltpu.VMEM((n_q, own_u, rank), bf),
            pltpu.VMEM((n_q, own_u, rank), bf),
            pltpu.VMEM((n_q, own_u, rank), bf),
            pltpu.VMEM((n_q, own_u, rank), bf),
            pltpu.VMEM((col_tiles, rank, tile), f32),
            pltpu.VMEM((n_r, own_v, rank), bf),
            pltpu.VMEM((n_r, own_v, rank), bf),
            pltpu.VMEM((8, tile), f32),
            pltpu.VMEM((n_r, 8, tile // 2), f32),
            pltpu.VMEM((n_c, 8, tile // 2), f32),
            dma((4,)),
            dma((n_r,)), dma((n_r,)),
            dma((n_q, CUTS)), dma((n_q, CUTS)), dma((n_q, CUTS)),
            dma((n_q, CUTS)), dma((n_q, CUTS)),
            dma((n_q,)), dma((n_q,)),
            dma((n_q,)), dma((n_q,)),
            dma((n_r,)), dma((n_r,)),
            dma((n_r,)), dma((n_r,)),
            dma((n_c,)), dma((n_c,)),
        ],
        compiler_params=pltpu.CompilerParams(collective_id=0, has_side_effects=True),
    )(factor_u, factor_v, values, mask_words, tile_cols)
    return new_u, new_v, loss[0, 0]


def solution(mesh):
    n_r, n_c = mesh.shape["rows"], mesh.shape["cols"]
    in_specs = (
        P("rows", "cols", None),
        P("cols", "rows", None),
        P("rows", "cols", None, None, None),
        P("rows", "cols", None, None, None),
        P("rows", "cols", None),
    )
    out_specs = (P("rows", "cols", None), P("cols", "rows", None), P())
    return jax.shard_map(
        functools.partial(per_device, n_r, n_c),
        mesh=mesh, in_specs=in_specs, out_specs=out_specs, check_vma=False,
    )
```
